32 devices in a mesh: seq: 4 (over z), grp: 8 (over y, x, core).
Axes of the slice: x: 2, y: 2, z: 4, core: 2. Of those that a mesh axis runs over, the one named last changes fastest.
Arguments:
- hidden_in: bfloat16 [8, 2048, 1024], P('grp', 'seq'), may hold values from -64 to 64, as said below
- lengths: int32 [8], P('grp'), may hold values from 256 to 2048
- project_weight: bfloat16 [1024, 3072], replicated, may hold values from -0.1875 to 0.1875
- output_weight: bfloat16 [1024, 1024], replicated, may hold values from -0.1875 to 0.1875
- first_gain: float32 [1024], replicated, may hold values from 0.5 to 1.5
- first_shift: float32 [1024], replicated, may hold values from -3 to 3
- up_weight: bfloat16 [1024, 4096], P('grp'), may hold values from -0.1875 to 0.1875
- down_weight: bfloat16 [1024, 4096], P('grp'), may hold values from -0.09375 to 0.09375
- second_gain: float32 [1024], replicated, may hold values from 0.5 to 1.5
- second_shift: float32 [1024], replicated, may hold values from -3 to 3
- queries: float32 [64, 1024], P('grp'), may hold values from -6 to 6
- positive: int32 [64], P('grp'), may hold values from 0 to 7
Outputs:
- hidden_out: bfloat16 [8, 2048, 1024], P('grp', 'seq')
- embeddings: float32 [8, 1024], P('grp')
- query_loss: float32 [64], P('grp')
The draws below stay inside these ranges and needn't reach their ends.
Inputs may be any that keep to these rules, and one draw needn't show every extreme that they name: `hidden_in`: activations.
All inputs are finite; a program needn't handle non-finite values.
Results may differ from the reference program's by a relative error of at most 0.0076.
Values may be sent and summed in bfloat16 or wider, within the bound.
A program may use at most 192 MiB of HBM per device.

```python
import math
import jax
import jax.numpy as jnp
from jax import lax

D = 1024
HEADS = 16
HEAD_DIM = 64
FF = 4096
LEN = 2048
PASSAGES = 8
QUERIES = 64


def draw_hidden_in(key, part):
    base = jnp.clip(jax.random.normal(key, (PASSAGES, LEN, D), jnp.float32), -6.0, 6.0)
    return base.astype(jnp.bfloat16)


def plant(drawn, own_key, least, high):
    spot = [jax.random.randint(jax.random.fold_in(own_key, axis), (), 0, length) for axis, length in enumerate(drawn.shape)]
    main_axis = drawn.shape.index(max(drawn.shape))
    neighbour = spot[:main_axis] + [(spot[main_axis] + 1) % drawn.shape[main_axis]] + spot[main_axis + 1:]
    return drawn.at[tuple(spot)].set(least).at[tuple(neighbour)].set(high)


def shard_levels(stream_key, dims, shards, low, top_value):
    def one(position, parts):
        draws = jax.random.uniform(jax.random.fold_in(jax.random.fold_in(stream_key, 6), position), (parts,), jnp.float32, low / len(shards), top_value / len(shards))
        return jnp.repeat(jnp.exp(draws), dims[position] // parts).reshape((-1,) + (1,) * (len(dims) - position - 1))

    factor_of = one(*shards[0])
    for cut in shards[1:]:
        factor_of = factor_of * one(*cut)
    return factor_of


def bell_draw(stream_key, dims, width, most, shards=(), kind=jnp.bfloat16):
    level = shard_levels(stream_key, dims, shards, -0.22, 0.18) if shards else 1.0
    values = jax.random.normal(stream_key, dims, jnp.float32) * width * level
    return jnp.minimum(jnp.maximum(values, -most), most).astype(kind)


def setup_inputs(seed: int = 0) -> dict:
    arg_keys = jax.random.split(jax.random.key(seed), 13)
    hidden_in = draw_hidden_in(jax.random.fold_in(arg_keys[12], 71), 0)
    lengths = plant(jax.random.randint(arg_keys[1], (PASSAGES,), LEN // 8, LEN + 1), jax.random.fold_in(arg_keys[1], 1), LEN // 8, LEN).astype(jnp.int32)
    project_weight = bell_draw(arg_keys[2], (D, 3 * D), D ** -0.5, 0.1875)
    output_weight = bell_draw(arg_keys[3], (D, D), D ** -0.5, 0.1875)
    first_gain = jnp.clip(1.0 + 0.1 * jax.random.normal(arg_keys[4], (D,), jnp.float32), 0.5, 1.5)
    first_shift = bell_draw(arg_keys[5], (D,), 0.5, 3.0, (), jnp.float32)
    up_weight = bell_draw(arg_keys[6], (D, FF), D ** -0.5, 0.1875, ((0, 8),))
    down_weight = bell_draw(arg_keys[7], (D, FF), FF ** -0.5, 0.09375, ((0, 8),))
    second_gain = jnp.clip(1.0 + 0.1 * jax.random.normal(arg_keys[8], (D,), jnp.float32), 0.5, 1.5)
    second_shift = bell_draw(arg_keys[9], (D,), 0.5, 3.0, (), jnp.float32)
    queries = bell_draw(arg_keys[10], (QUERIES, D), 1.0, 6.0, ((0, 8),), jnp.float32)
    positive = plant(jax.random.randint(arg_keys[11], (QUERIES,), 0, PASSAGES), jax.random.fold_in(arg_keys[11], 1), 0, PASSAGES - 1).astype(jnp.int32)
    return {"hidden_in": hidden_in, "lengths": lengths, "project_weight": project_weight, "output_weight": output_weight, "first_gain": first_gain, "first_shift": first_shift, "up_weight": up_weight, "down_weight": down_weight, "second_gain": second_gain, "second_shift": second_shift, "queries": queries, "positive": positive}


def layer_norm(values, gain, shift):
    average = lax.optimization_barrier(jnp.mean(values, axis=-1, keepdims=True))
    centred = values - average
    variance = lax.optimization_barrier(jnp.mean(centred * centred, axis=-1, keepdims=True))
    return centred * lax.rsqrt(variance + 1e-05) * gain + shift

def attend(projected, length):
    block = min(1024, LEN)
    query_all = projected[:, :D].reshape(LEN, HEADS, HEAD_DIM).astype(jnp.float32)
    key_all = projected[:, D:2 * D].reshape(LEN, HEADS, HEAD_DIM).astype(jnp.float32)
    value_all = projected[:, 2 * D:].reshape(LEN, HEADS, HEAD_DIM).astype(jnp.float32)
    key_valid = jnp.arange(LEN, dtype=jnp.int32) < length
    scale = 1.0 / math.sqrt(HEAD_DIM)

    def one_block(index):
        query_rows = lax.dynamic_slice_in_dim(query_all, (index * block).astype(jnp.int32), block, 0)
        scores = jnp.einsum('qhd,khd->hqk', query_rows, key_all) * scale
        scores = jnp.where(key_valid[None, None, :], scores, -jnp.inf)
        highest = lax.optimization_barrier(jnp.max(scores, axis=-1, keepdims=True))
        expo = jnp.exp(scores - highest)
        probs = (expo / lax.optimization_barrier(jnp.sum(expo, axis=-1, keepdims=True))).astype(jnp.bfloat16)
        result = jnp.einsum('hqk,khd->qhd', probs.astype(jnp.float32), value_all)
        return result.astype(jnp.bfloat16).reshape(block, D)
    blocks = lax.map(one_block, jnp.arange(LEN // block, dtype=jnp.int32))
    return blocks.reshape(LEN, D)

def reference(hidden_in, lengths, project_weight, output_weight, first_gain, first_shift, up_weight, down_weight, second_gain, second_shift, queries, positive):

    def encode(item):
        tokens, length = item
        projected = jnp.dot(tokens, project_weight, preferred_element_type=jnp.float32).astype(jnp.bfloat16)
        attended = attend(projected, length)
        mixed = jnp.dot(attended, output_weight, preferred_element_type=jnp.float32) + tokens.astype(jnp.float32)
        normed = layer_norm(mixed, first_gain, first_shift).astype(jnp.bfloat16)
        inner = jax.nn.gelu(jnp.dot(normed, up_weight, preferred_element_type=jnp.float32), approximate=False).astype(jnp.bfloat16)
        outer = lax.dot_general(inner, down_weight, (((1,), (1,)), ((), ())), preferred_element_type=jnp.float32)
        final = layer_norm(outer + normed.astype(jnp.float32), second_gain, second_shift)
        valid = (jnp.arange(LEN, dtype=jnp.int32) < length).astype(jnp.float32)
        pooled = lax.optimization_barrier(jnp.sum(final * valid[:, None], axis=0)) / length.astype(jnp.float32)
        return (final.astype(jnp.bfloat16), pooled)
    hidden_out, pooled = lax.map(encode, (hidden_in, lengths))
    embeddings = pooled / jnp.sqrt(lax.optimization_barrier(jnp.sum(pooled * pooled, axis=-1, keepdims=True)) + 1e-06)
    short_queries = (queries / jnp.sqrt(lax.optimization_barrier(jnp.sum(queries * queries, axis=-1, keepdims=True)) + 1e-06)).astype(jnp.bfloat16)
    short_passages = embeddings.astype(jnp.bfloat16)
    logits = 20.0 * jnp.dot(short_queries, short_passages.T, preferred_element_type=jnp.float32)
    chosen = positive[:, None] == jnp.arange(PASSAGES, dtype=jnp.int32)[None, :]
    picked = lax.optimization_barrier(jnp.sum(jnp.where(chosen, logits, 0.0), axis=1))
    query_loss = jnp.log(lax.optimization_barrier(jnp.sum(jnp.exp(logits), axis=1))) - picked
    return (hidden_out, embeddings, query_loss)
```

```python
import functools
import math

import jax
import jax.numpy as jnp
from jax import lax
from jax.experimental import pallas as pl
from jax.experimental.pallas import tpu as pltpu
from jax.sharding import PartitionSpec as P

HEAD_DIM = 64
PAIR = 2 * HEAD_DIM
LOW = -1e30


def layer_norm(values, gain, shift):
    average = jnp.mean(values, axis=-1, keepdims=True)
    centred = values - average
    variance = jnp.mean(centred * centred, axis=-1, keepdims=True)
    return centred * lax.rsqrt(variance + 1e-05) * gain + shift


def attend_kernel(first, last, *refs):
    place, query_ref, key_ref, value_ref = refs[:4]
    refs = refs[4:]
    if first:
        acc_in = stat_in = None
    else:
        acc_in, stat_in = refs[:2]
        refs = refs[2:]
    start, length = place[0], place[1]
    rows = query_ref.shape[0]
    keys = key_ref.shape[0]
    lane = lax.broadcasted_iota(jnp.int32, (1, PAIR), 1)
    left = lane < HEAD_DIM

    def emit(total, highs, sums):
        if last:
            refs[0][...] = (total / jnp.where(left, sums[0], sums[1])).astype(jnp.bfloat16)
        else:
            refs[0][0] = total
            high = jnp.where(left, highs[0], highs[1])
            summed = jnp.where(left, sums[0], sums[1])
            refs[1][0] = jnp.where(lax.rem(lane, HEAD_DIM) < HEAD_DIM // 2, high, summed)

    def before():
        if first:
            return None, (jnp.full((rows, 1), LOW, jnp.float32),) * 2, (jnp.zeros((rows, 1), jnp.float32),) * 2
        half = HEAD_DIM // 2
        highs = tuple(stat_in[0, :, i * HEAD_DIM : i * HEAD_DIM + 1] for i in range(2))
        sums = tuple(stat_in[0, :, i * HEAD_DIM + half : i * HEAD_DIM + half + 1] for i in range(2))
        return acc_in[0], highs, sums

    def work(masked):
        total, highs, sums = before()
        query = query_ref[...]
        key = key_ref[...]
        value = value_ref[...]
        outs, alphas, new_highs, new_sums = [], [], [], []
        for head in range(2):
            mine = left if head == 0 else jnp.logical_not(left)
            keep = jnp.where(mine, 1.0, 0.0).astype(jnp.bfloat16)
            other = jnp.where(mine, 0.0, 1.0).astype(jnp.bfloat16)
            scores = lax.dot_general(
                query * keep, key, (((1,), (1,)), ((), ())), preferred_element_type=jnp.float32
            )
            if masked:
                column = lax.broadcasted_iota(jnp.int32, (1, keys), 1) + start
                scores = jnp.where(column < length, scores, LOW)
            high = jnp.max(scores, axis=1, keepdims=True)
            if not first:
                high = jnp.maximum(high, highs[head])
            expo = jnp.exp2(scores - high).astype(jnp.bfloat16)
            out = jnp.dot(expo, value * keep + other, preferred_element_type=jnp.float32)
            at = HEAD_DIM * (1 - head)
            summed = out[:, at : at + 1]
            if not first:
                alpha = jnp.exp2(highs[head] - high)
                alphas.append(alpha)
                summed = summed + alpha * sums[head]
            outs.append(out)
            new_highs.append(high)
            new_sums.append(summed)
        new_total = jnp.where(left, outs[0], outs[1])
        if not first:
            new_total = new_total + total * jnp.where(left, alphas[0], alphas[1])
        emit(new_total, new_highs, new_sums)

    @pl.when(start + keys <= length)
    def _():
        work(False)

    @pl.when(jnp.logical_and(start < length, start + keys > length))
    def _():
        work(True)

    @pl.when(start >= length)
    def _():
        total, highs, sums = before()
        if first:
            total = jnp.zeros((rows, PAIR), jnp.float32)
        emit(total, highs, sums)


def attend_stage(place, query, key_value, carry, last):
    rows, width = query.shape
    keys = key_value.shape[0]
    pairs = width // PAIR
    first = carry is None
    state_spec = pl.BlockSpec((1, rows, PAIR), lambda p, s: (p, 0, 0))
    in_specs = [
        pl.BlockSpec((rows, PAIR), lambda p, s: (0, p)),
        pl.BlockSpec((keys, PAIR), lambda p, s: (0, p)),
        pl.BlockSpec((keys, PAIR), lambda p, s: (0, pairs + p)),
    ]
    args = [place, query, key_value, key_value]
    if not first:
        in_specs += [state_spec, state_spec]
        args += list(carry)
    if last:
        out_specs = pl.BlockSpec((rows, PAIR), lambda p, s: (0, p))
        out_shape = jax.ShapeDtypeStruct((rows, width), jnp.bfloat16)
    else:
        out_specs = [state_spec, state_spec]
        out_shape = [jax.ShapeDtypeStruct((pairs, rows, PAIR), jnp.float32)] * 2
    return pl.pallas_call(
        functools.partial(attend_kernel, first, last),
        grid_spec=pltpu.PrefetchScalarGridSpec(
            num_scalar_prefetch=1, grid=(pairs,), in_specs=in_specs, out_specs=out_specs
        ),
        out_shape=out_shape,
        cost_estimate=pl.CostEstimate(
            flops=8 * rows * keys * width,
            bytes_accessed=16 * rows * width,
            transcendentals=rows * keys * width // HEAD_DIM,
        ),
        compiler_params=pltpu.CompilerParams(vmem_limit_bytes=32 * 1024 * 1024),
    )(*args)


def chain(block, size):
    lower, upper = [block], [block]
    for step in range(1, size):
        up_pairs = [(j, j + 1) for j in range(step - 1, size - 1)]
        down_pairs = [(j + 1, j) for j in range(0, size - step)]
        lower.append(lax.ppermute(lower[-1], "seq", up_pairs))
        upper.append(lax.ppermute(upper[-1], "seq", down_pairs))
    return lower, upper


def stage_plan(rank, size, stage):
    if stage == 0:
        return True, 0
    near = min(rank, size - 1 - rank)
    if stage <= 2 * near:
        return stage % 2 == 1, (stage + 1) // 2
    return rank > size - 1 - rank, stage - near


def stage_block(rank, size, stage, lower, upper):
    plans = [stage_plan(r, size, stage) for r in range(size)]
    kinds = sorted(set(plans))
    choice = jnp.array([kinds.index(p) for p in plans], jnp.int32)[rank]
    owner = jnp.array(
        [r - d if below else r + d for r, (below, d) in enumerate(plans)], jnp.int32
    )[rank]
    cases = [(lower if below else upper)[d] for below, d in kinds]
    block = cases[0]
    for index, case in enumerate(cases[1:], 1):
        block = jnp.where(choice == index, case, block)
    return block, owner


def swap(value, size, bit):
    return lax.ppermute(value, "grp", [(g, g ^ bit) for g in range(size)])


def weight_parts(part, size):
    half = part.shape[0] // 2
    across_x = swap(part, size, 2)
    across_y = swap(part, size, 4)
    corner = jnp.concatenate(
        [swap(across_y[:half], size, 2), swap(across_x[half:], size, 4)], axis=0
    )
    even = [part, across_x, across_y, corner]
    odd = [swap(value, size, 1) for value in even]
    return [value for both in zip(even, odd) for value in both]


def regroup(values, group, size):
    width = values.shape[1] // size
    return jnp.concatenate(
        [
            lax.dynamic_slice_in_dim(values, lax.bitwise_xor(group, d) * width, width, 1)
            for d in range(size)
        ],
        axis=1,
    )


def body(
    seq_size,
    grp_size,
    hidden_in,
    lengths,
    project_weight,
    output_weight,
    first_gain,
    first_shift,
    up_weight,
    down_weight,
    second_gain,
    second_shift,
    queries,
    positive,
):
    tokens = hidden_in[0]
    tok_rows, width = tokens.shape
    rank = lax.axis_index("seq")
    group = lax.axis_index("grp")
    length = lengths[0]
    by_swaps = grp_size == 8

    lower, upper = chain(tokens, seq_size)
    if by_swaps:
        up_full = jnp.concatenate(weight_parts(up_weight, grp_size), axis=0)
        down_full = jnp.concatenate(weight_parts(down_weight, grp_size), axis=0)
    else:
        up_full = lax.all_gather(up_weight, "grp", axis=0, tiled=True)
        down_full = lax.all_gather(down_weight, "grp", axis=0, tiled=True)

    factor = math.log2(math.e) / math.sqrt(HEAD_DIM)
    query = (
        jnp.dot(tokens, project_weight[:, :width], preferred_element_type=jnp.float32) * factor
    ).astype(jnp.bfloat16)
    carry = None
    for stage in range(seq_size):
        block, owner = stage_block(rank, seq_size, stage, lower, upper)
        key_value = jnp.dot(
            block, project_weight[:, width:], preferred_element_type=jnp.float32
        ).astype(jnp.bfloat16)
        place = jnp.stack([owner * tok_rows, length])
        carry = attend_stage(place, query, key_value, carry, stage == seq_size - 1)
    mixed = jnp.dot(carry, output_weight, preferred_element_type=jnp.float32)
    mixed = mixed + tokens.astype(jnp.float32)
    normed = layer_norm(mixed, first_gain, first_shift).astype(jnp.bfloat16)

    rows_in = regroup(normed, group, grp_size) if by_swaps else normed
    inner = jax.nn.gelu(
        jnp.dot(rows_in, up_full, preferred_element_type=jnp.float32), approximate=False
    ).astype(jnp.bfloat16)
    outer = lax.dot_general(
        inner, down_full, (((1,), (1,)), ((), ())), preferred_element_type=jnp.float32
    )
    if by_swaps:
        outer = regroup(outer, group, grp_size)
    final = layer_norm(outer + normed.astype(jnp.float32), second_gain, second_shift)
    position = rank * tok_rows + jnp.arange(tok_rows, dtype=jnp.int32)
    valid = (position < length).astype(jnp.float32)
    local_total = jnp.sum(final * valid[:, None], axis=0) / length.astype(jnp.float32)
    parts = lax.all_gather(local_total, ("grp", "seq"), axis=0, tiled=False)
    pooled = jnp.sum(parts.reshape(grp_size, seq_size, width), axis=1)
    passages = pooled / jnp.sqrt(jnp.sum(pooled * pooled, axis=-1, keepdims=True) + 1e-06)
    embedding = lax.dynamic_slice_in_dim(passages, group, 1, 0)
    short_passages = passages.astype(jnp.bfloat16)
    short_queries = (
        queries / jnp.sqrt(jnp.sum(queries * queries, axis=-1, keepdims=True) + 1e-06)
    ).astype(jnp.bfloat16)
    logits = 20.0 * jnp.dot(short_queries, short_passages.T, preferred_element_type=jnp.float32)
    passage_ids = jnp.arange(grp_size, dtype=jnp.int32)
    chosen = positive[:, None] == passage_ids[None, :]
    picked = jnp.sum(jnp.where(chosen, logits, 0.0), axis=1)
    query_loss = jnp.log(jnp.sum(jnp.exp(logits), axis=1)) - picked
    return (final.astype(jnp.bfloat16)[None], embedding, query_loss)


def solution(mesh):
    in_specs = (
        P("grp", "seq", None),
        P("grp"),
        P(),
        P(),
        P(),
        P(),
        P("grp", None),
        P("grp", None),
        P(),
        P(),
        P("grp", None),
        P("grp"),
    )
    out_specs = (P("grp", "seq", None), P("grp", None), P("grp"))
    sized = functools.partial(body, mesh.shape["seq"], mesh.shape["grp"])
    return jax.shard_map(sized, mesh=mesh, in_specs=in_specs, out_specs=out_specs, check_vma=False)
```

```python
import functools
import math

import jax
import jax.numpy as jnp
from jax import lax
from jax.experimental import pallas as pl
from jax.experimental.pallas import tpu as pltpu
from jax.sharding import PartitionSpec as P

HEAD_DIM = 64
PAIR = 2 * HEAD_DIM
LOW = -1e30


def layer_norm(values, gain, shift):
    average = jnp.mean(values, axis=-1, keepdims=True)
    centred = values - average
    variance = jnp.mean(centred * centred, axis=-1, keepdims=True)
    return centred * lax.rsqrt(variance + 1e-05) * gain + shift


def attend_kernel(first, last, *refs):
    place, query_ref, key_ref, value_ref = refs[:4]
    refs = refs[4:]
    if not first:
        acc_in, high_in, sum_in = refs[:3]
        refs = refs[3:]
    start, length = place[0], place[1]
    rows = query_ref.shape[0]
    keys = key_ref.shape[0]
    lane = lax.broadcasted_iota(jnp.int32, (1, PAIR), 1)
    left = lane < HEAD_DIM

    def emit(total, high, summed):
        if last:
            refs[0][...] = (total / summed).astype(jnp.bfloat16)
        else:
            refs[0][0] = total
            refs[1][0] = high
            refs[2][0] = summed

    def work(masked):
        query = query_ref[...]
        key = key_ref[...]
        value = value_ref[...]
        outs, highs = [], []
        for head in range(2):
            mine = left if head == 0 else jnp.logical_not(left)
            keep = jnp.where(mine, 1.0, 0.0).astype(jnp.bfloat16)
            other = jnp.where(mine, 0.0, 1.0).astype(jnp.bfloat16)
            scores = lax.dot_general(
                query * keep, key, (((1,), (1,)), ((), ())), preferred_element_type=jnp.float32
            )
            if masked:
                column = lax.broadcasted_iota(jnp.int32, (1, keys), 1) + start
                scores = jnp.where(column < length, scores, LOW)
            high = jnp.max(scores, axis=1, keepdims=True)
            if not first:
                at = HEAD_DIM * head
                high = jnp.maximum(high, high_in[0, :, at : at + 1])
            expo = jnp.exp2(scores - high).astype(jnp.bfloat16)
            outs.append(jnp.dot(expo, value * keep + other, preferred_element_type=jnp.float32))
            highs.append(high)
        total = jnp.where(left, outs[0], outs[1])
        summed = pltpu.roll(jnp.where(left, outs[1], outs[0]), HEAD_DIM, 1)
        high = jnp.where(left, highs[0], highs[1])
        if not first:
            alpha = jnp.exp2(high_in[0] - high)
            total = total + acc_in[0] * alpha
            summed = summed + sum_in[0] * alpha
        emit(total, high, summed)

    @pl.when(start + keys <= length)
    def _():
        work(False)

    @pl.when(jnp.logical_and(start < length, start + keys > length))
    def _():
        work(True)

    @pl.when(start >= length)
    def _():
        if first:
            zero = jnp.zeros((rows, PAIR), jnp.float32)
            emit(zero, zero + LOW, zero)
        else:
            emit(acc_in[0], high_in[0], sum_in[0])


def attend_stage(place, query, key_value, carry, last):
    rows, width = query.shape
    keys = key_value.shape[0]
    pairs = width // PAIR
    first = carry is None
    state_spec = pl.BlockSpec((1, rows, PAIR), lambda p, s: (p, 0, 0))
    in_specs = [
        pl.BlockSpec((rows, PAIR), lambda p, s: (0, p)),
        pl.BlockSpec((keys, PAIR), lambda p, s: (0, p)),
        pl.BlockSpec((keys, PAIR), lambda p, s: (0, pairs + p)),
    ]
    args = [place, query, key_value, key_value]
    if not first:
        in_specs += [state_spec] * 3
        args += list(carry)
    if last:
        out_specs = pl.BlockSpec((rows, PAIR), lambda p, s: (0, p))
        out_shape = jax.ShapeDtypeStruct((rows, width), jnp.bfloat16)
    else:
        out_specs = [state_spec] * 3
        out_shape = [jax.ShapeDtypeStruct((pairs, rows, PAIR), jnp.float32)] * 3
    return pl.pallas_call(
        functools.partial(attend_kernel, first, last),
        grid_spec=pltpu.PrefetchScalarGridSpec(
            num_scalar_prefetch=1, grid=(pairs,), in_specs=in_specs, out_specs=out_specs
        ),
        out_shape=out_shape,
        cost_estimate=pl.CostEstimate(
            flops=8 * rows * keys * width,
            bytes_accessed=16 * rows * width,
            transcendentals=rows * keys * width // HEAD_DIM,
        ),
        compiler_params=pltpu.CompilerParams(vmem_limit_bytes=32 * 1024 * 1024),
    )(*args)


def chain(block, size):
    lower, upper = [block], [block]
    for step in range(1, size):
        up_pairs = [(j, j + 1) for j in range(step - 1, size - 1)]
        down_pairs = [(j + 1, j) for j in range(0, size - step)]
        lower.append(lax.ppermute(lower[-1], "seq", up_pairs))
        upper.append(lax.ppermute(upper[-1], "seq", down_pairs))
    return lower, upper


def stage_plan(rank, size, stage):
    if stage == 0:
        return True, 0
    near = min(rank, size - 1 - rank)
    if stage <= 2 * near:
        return stage % 2 == 1, (stage + 1) // 2
    return rank > size - 1 - rank, stage - near


def stage_block(rank, size, stage, lower, upper):
    plans = [stage_plan(r, size, stage) for r in range(size)]
    kinds = sorted(set(plans))
    choice = jnp.array([kinds.index(p) for p in plans], jnp.int32)[rank]
    owner = jnp.array(
        [r - d if below else r + d for r, (below, d) in enumerate(plans)], jnp.int32
    )[rank]
    cases = [(lower if below else upper)[d] for below, d in kinds]
    block = cases[0]
    for index, case in enumerate(cases[1:], 1):
        block = jnp.where(choice == index, case, block)
    return block, owner


def body(
    seq_size,
    grp_size,
    hidden_in,
    lengths,
    project_weight,
    output_weight,
    first_gain,
    first_shift,
    up_weight,
    down_weight,
    second_gain,
    second_shift,
    queries,
    positive,
):
    tokens = hidden_in[0]
    tok_rows, width = tokens.shape
    rank = lax.axis_index("seq")
    length = lengths[0]

    lower, upper = chain(tokens, seq_size)
    up_full = lax.all_gather(up_weight, "grp", axis=0, tiled=True)
    down_full = lax.all_gather(down_weight, "grp", axis=0, tiled=True)

    factor = math.log2(math.e) / math.sqrt(HEAD_DIM)
    query = (
        jnp.dot(tokens, project_weight[:, :width], preferred_element_type=jnp.float32) * factor
    ).astype(jnp.bfloat16)
    carry = None
    for stage in range(seq_size):
        block, owner = stage_block(rank, seq_size, stage, lower, upper)
        key_value = jnp.dot(
            block, project_weight[:, width:], preferred_element_type=jnp.float32
        ).astype(jnp.bfloat16)
        place = jnp.stack([owner * tok_rows, length])
        carry = attend_stage(place, query, key_value, carry, stage == seq_size - 1)
    mixed = jnp.dot(carry, output_weight, preferred_element_type=jnp.float32)
    mixed = mixed + tokens.astype(jnp.float32)
    normed = layer_norm(mixed, first_gain, first_shift).astype(jnp.bfloat16)

    inner = jax.nn.gelu(
        jnp.dot(normed, up_full, preferred_element_type=jnp.float32), approximate=False
    ).astype(jnp.bfloat16)
    outer = lax.dot_general(
        inner, down_full, (((1,), (1,)), ((), ())), preferred_element_type=jnp.float32
    )
    final = layer_norm(outer + normed.astype(jnp.float32), second_gain, second_shift)
    position = rank * tok_rows + jnp.arange(tok_rows, dtype=jnp.int32)
    valid = (position < length).astype(jnp.float32)
    local_total = jnp.sum(final * valid[:, None], axis=0)
    pooled = lax.psum(local_total, "seq") / length.astype(jnp.float32)
    embedding = pooled / jnp.sqrt(jnp.sum(pooled * pooled) + 1e-06)
    short_passages = lax.all_gather(
        embedding.astype(jnp.bfloat16)[None, :], "grp", axis=0, tiled=True
    )
    short_queries = (
        queries / jnp.sqrt(jnp.sum(queries * queries, axis=-1, keepdims=True) + 1e-06)
    ).astype(jnp.bfloat16)
    logits = 20.0 * jnp.dot(short_queries, short_passages.T, preferred_element_type=jnp.float32)
    passage_ids = jnp.arange(grp_size, dtype=jnp.int32)
    chosen = positive[:, None] == passage_ids[None, :]
    picked = jnp.sum(jnp.where(chosen, logits, 0.0), axis=1)
    query_loss = jnp.log(jnp.sum(jnp.exp(logits), axis=1)) - picked
    return (final.astype(jnp.bfloat16)[None], embedding[None, :], query_loss)


def solution(mesh):
    in_specs = (
        P("grp", "seq", None),
        P("grp"),
        P(),
        P(),
        P(),
        P(),
        P("grp", None),
        P("grp", None),
        P(),
        P(),
        P("grp", None),
        P("grp"),
    )
    out_specs = (P("grp", "seq", None), P("grp", None), P("grp"))
    sized = functools.partial(body, mesh.shape["seq"], mesh.shape["grp"])
    return jax.shard_map(sized, mesh=mesh, in_specs=in_specs, out_specs=out_specs, check_vma=False)
```
